32 devices in a mesh: dp: 2 (over x), col: 4 (over z), row: 4 (over y, core).
Axes of the slice: x: 2, y: 2, z: 4, core: 2. Of those that a mesh axis runs over, the one named last changes fastest.
Arguments:
- x_in: bfloat16 [2048, 5120], P(('dp', 'row'), 'col'), parts along dimension 0
- w_qkv: bfloat16 [5120, 15360], P('row', 'col')
- w_out: bfloat16 [5120, 5120], P('row', 'col')
- doc_ids: int32 [2048], P(('dp', 'row')), parts along dimension 0
- grad_y: bfloat16 [2048, 5120], P(('dp', 'row'), 'col'), parts along dimension 0
Outputs:
- output 1: bfloat16 [2048, 5120], P(('dp', 'row'), 'col'), parts along dimension 0
- output 2: bfloat16 [10240, 15360], P(('dp', 'row'), 'col'), parts along dimension 0
- output 3: bfloat16 [10240, 5120], P(('dp', 'row'), 'col'), parts along dimension 0
There are 2 independent parts. The reference program is written for one: setup_inputs(seed, part) draws one part's arguments, and reference() takes and returns one part's arrays. A program takes and returns all parts, laid end to end along the dimension named above; an argument that names none is the same for every part.
All inputs are finite; a program needn't handle non-finite values.
Results may differ from the reference program's by a relative error of at most 0.00412.
Values are sent between devices in bfloat16 or wider.
A program may use at most 1 GiB of HBM per device.

```python
import jax
import jax.numpy as jnp
from jax import lax

TOKENS = 1024
HIDDEN = 5120
HEADS = 40
HEAD_DIM = 128
QUERY_BLOCK = 256
DOCS = 3


def setup_inputs(seed: int = 0, part: int = 0) -> dict:
    part_key = jax.random.fold_in(jax.random.key(seed), part)
    key_x, key_doc, key_dy = jax.random.split(part_key, 3)
    key_wq, key_wo = jax.random.split(jax.random.key(seed + 1), 2)
    x_in = jax.random.normal(key_x, (TOKENS, HIDDEN), jnp.float32).astype(jnp.bfloat16)
    w_qkv = (jax.random.normal(key_wq, (HIDDEN, 3 * HIDDEN), jnp.float32) * HIDDEN ** -0.5).astype(jnp.bfloat16)
    w_out = (jax.random.normal(key_wo, (HIDDEN, HIDDEN), jnp.float32) * HIDDEN ** -0.5).astype(jnp.bfloat16)
    doc_cuts = jax.random.randint(key_doc, (DOCS - 1,), 1, TOKENS)
    doc_ids = jnp.sum(jnp.arange(TOKENS)[:, None] >= doc_cuts[None, :], axis=1).astype(jnp.int32)
    grad_y = jax.random.normal(key_dy, (TOKENS, HIDDEN), jnp.float32).astype(jnp.bfloat16)
    return {'x_in': x_in, 'w_qkv': w_qkv, 'w_out': w_out, 'doc_ids': doc_ids, 'grad_y': grad_y}


def reference(x_in, w_qkv, w_out, doc_ids, grad_y):
    sm_scale = HEAD_DIM ** -0.5
    n_blocks = TOKENS // QUERY_BLOCK
    qkv_all = jnp.dot(x_in, w_qkv, preferred_element_type=jnp.float32).astype(jnp.bfloat16)
    qkv_heads = jnp.transpose(qkv_all.reshape(TOKENS, HEADS, 3, HEAD_DIM), (1, 2, 0, 3))
    d_attn = jnp.dot(grad_y, w_out.T, preferred_element_type=jnp.float32).astype(jnp.bfloat16)
    dattn_heads = jnp.transpose(d_attn.reshape(TOKENS, HEADS, HEAD_DIM), (1, 0, 2))
    seg_blocks = doc_ids.reshape(n_blocks, QUERY_BLOCK)

    def one_head(head_args):
        qkv_head, do_head = head_args
        q_head = qkv_head[0]
        k_head = qkv_head[1]
        v_head = qkv_head[2]

        def one_block(acc_pair, blk_args):
            dk_acc, dv_acc = acc_pair
            q_blk, do_blk, seg_blk = blk_args
            scores = jnp.dot(q_blk, k_head.T, preferred_element_type=jnp.float32) * sm_scale
            scores = jnp.where(seg_blk[:, None] == doc_ids[None, :], scores, -jnp.inf)
            p_attn = jax.nn.softmax(scores, axis=-1)
            p_bf = p_attn.astype(jnp.bfloat16)
            o_blk = jnp.dot(p_bf, v_head, preferred_element_type=jnp.float32).astype(jnp.bfloat16)
            d_probs = jnp.dot(do_blk, v_head.T, preferred_element_type=jnp.float32)
            row_dot = jnp.sum(p_attn * d_probs, axis=-1, keepdims=True)
            d_scores = (p_attn * (d_probs - row_dot) * sm_scale).astype(jnp.bfloat16)
            dq_blk = jnp.dot(d_scores, k_head, preferred_element_type=jnp.float32)
            dk_acc = dk_acc + jnp.dot(d_scores.T, q_blk, preferred_element_type=jnp.float32)
            dv_acc = dv_acc + jnp.dot(p_bf.T, do_blk, preferred_element_type=jnp.float32)
            return (dk_acc, dv_acc), (o_blk, dq_blk)

        zero_acc = jnp.zeros((TOKENS, HEAD_DIM), jnp.float32)
        blk_inputs = (q_head.reshape(n_blocks, QUERY_BLOCK, HEAD_DIM), do_head.reshape(n_blocks, QUERY_BLOCK, HEAD_DIM), seg_blocks)
        (dk_head, dv_head), (o_head, dq_head) = lax.scan(one_block, (zero_acc, zero_acc), blk_inputs)
        dqkv_head = jnp.stack([dq_head.reshape(TOKENS, HEAD_DIM), dk_head, dv_head])
        return o_head.reshape(TOKENS, HEAD_DIM), dqkv_head

    attn_heads, dqkv_heads = lax.map(one_head, (qkv_heads, dattn_heads))
    attn_out = jnp.transpose(attn_heads, (1, 0, 2)).reshape(TOKENS, HIDDEN)
    d_qkv = jnp.transpose(dqkv_heads, (2, 0, 1, 3)).reshape(TOKENS, 3 * HIDDEN).astype(jnp.bfloat16)
    grad_x = jnp.dot(d_qkv, w_qkv.T, preferred_element_type=jnp.float32).astype(jnp.bfloat16)
    grad_wqkv = jnp.dot(x_in.T, d_qkv, preferred_element_type=jnp.float32).astype(jnp.bfloat16)
    grad_wout = jnp.dot(attn_out.T, grad_y, preferred_element_type=jnp.float32).astype(jnp.bfloat16)
    return (grad_x, grad_wqkv, grad_wout)
```

```python
import jax
import jax.numpy as jnp
from jax import lax
from jax.experimental import pallas as pl
from jax.experimental.pallas import tpu as pltpu
from jax.sharding import PartitionSpec as P


HEAD_DIM = 128
QUERY_STEP = 256
NT = (((1,), (1,)), ((), ()))
TN = (((0,), (0,)), ((), ()))
NN = (((1,), (0,)), ((), ()))


def mm(a, b, dims):
    return lax.dot_general(a, b, dims, preferred_element_type=jnp.float32)


def softmax(q, k, same):
    s = mm(q, k, NT) * HEAD_DIM ** -0.5
    s = jnp.where(same, s, -jnp.inf)
    e = jnp.exp(s - jnp.max(s, axis=-1, keepdims=True))
    return e / jnp.sum(e, axis=-1, keepdims=True)


def fwd_kernel(q_ref, k1_ref, v1_ref, k2_ref, v2_ref, sq_ref, sk_ref, o_ref):
    k = jnp.concatenate([k1_ref[...], k2_ref[...]], axis=0)
    v = jnp.concatenate([v1_ref[...], v2_ref[...]], axis=0)
    for i in range(q_ref.shape[0] // QUERY_STEP):
        rows = pl.ds(i * QUERY_STEP, QUERY_STEP)
        p = softmax(q_ref[rows, :], k, sq_ref[rows, :] == sk_ref[...])
        o_ref[rows, :] = mm(p.astype(jnp.bfloat16), v, NN).astype(jnp.bfloat16)


def bwd_kernel(q_ref, k1_ref, v1_ref, k2_ref, v2_ref, sq_ref, sk_ref, do_ref, dq_ref, own_ref, sib_ref):
    half = k1_ref.shape[0]
    k = jnp.concatenate([k1_ref[...], k2_ref[...]], axis=0)
    v = jnp.concatenate([v1_ref[...], v2_ref[...]], axis=0)
    dk = dv = None
    for i in range(q_ref.shape[0] // QUERY_STEP):
        rows = pl.ds(i * QUERY_STEP, QUERY_STEP)
        q = q_ref[rows, :]
        do = do_ref[rows, :]
        p = softmax(q, k, sq_ref[rows, :] == sk_ref[...])
        dp = mm(do, v, NT)
        dot = jnp.sum(p * dp, axis=-1, keepdims=True)
        ds = (p * (dp - dot) * HEAD_DIM ** -0.5).astype(jnp.bfloat16)
        dq_ref[rows, :] = mm(ds, k, NN).astype(jnp.bfloat16)
        dk_i = mm(ds, q, TN)
        dv_i = mm(p.astype(jnp.bfloat16), do, TN)
        dk = dk_i if dk is None else dk + dk_i
        dv = dv_i if dv is None else dv + dv_i
    own_ref[:, :HEAD_DIM] = dk[:half]
    own_ref[:, HEAD_DIM:] = dv[:half]
    sib_ref[:, :HEAD_DIM] = dk[half:]
    sib_ref[:, HEAD_DIM:] = dv[half:]


def attention(kernel, qkv, qkv_sib, seg_q, seg_k, do=None):
    n_tok, n_head = qkv.shape[0], qkv.shape[1] // (3 * HEAD_DIM)
    width = n_head * HEAD_DIM

    def col(off):
        return pl.BlockSpec((n_tok, HEAD_DIM), lambda h: (0, 3 * h + off))

    head = pl.BlockSpec((n_tok, HEAD_DIM), lambda h: (0, h))
    pair = pl.BlockSpec((n_tok, 2 * HEAD_DIM), lambda h: (0, h))
    in_specs = [
        col(0), col(1), col(2), col(1), col(2),
        pl.BlockSpec((n_tok, 1), lambda h: (0, 0)),
        pl.BlockSpec((1, 2 * n_tok), lambda h: (0, 0)),
    ]
    args = [qkv, qkv, qkv, qkv_sib, qkv_sib, seg_q, seg_k]
    narrow = jax.ShapeDtypeStruct((n_tok, width), jnp.bfloat16)
    wide = jax.ShapeDtypeStruct((n_tok, 2 * width), jnp.float32)
    out_specs, out_shape, products = [head], [narrow], 2
    if do is not None:
        in_specs.append(head)
        args.append(do)
        out_specs, out_shape, products = [head, pair, pair], [narrow, wide, wide], 5
    return pl.pallas_call(
        kernel,
        grid=(n_head,),
        in_specs=in_specs,
        out_specs=out_specs,
        out_shape=out_shape,
        compiler_params=pltpu.CompilerParams(vmem_limit_bytes=48 * 1024 * 1024),
        cost_estimate=pl.CostEstimate(
            flops=8 * products * n_tok * n_tok * width,
            bytes_accessed=12 * n_tok * width,
            transcendentals=2 * n_tok * n_tok * n_head,
        ),
    )(*args)


def solution(mesh):
    tok_spec = P(('dp', 'row'), 'col')
    mat_spec = P('row', 'col')
    seg_spec = P(('dp', 'row'))
    bf16 = jnp.bfloat16

    def to_row(v, j):
        return lax.ppermute(v, 'row', [(i, i ^ j) for i in range(4)])

    def to_other_group(v):
        return lax.ppermute(v, 'dp', [(0, 1), (1, 0)])

    mirror = (0, 2, 1, 3)

    def turn(v, j):
        pairs = [(c * 4 + r, r * 4 + ((r ^ mirror[c]) ^ j)) for c in range(4) for r in range(4)]
        return lax.ppermute(v, ('col', 'row'), pairs)

    def cols(v, start, size):
        return lax.dynamic_slice_in_dim(v, start, size, axis=1)

    def swap(v):
        half = v.shape[0] // 2
        return jnp.concatenate([v[half:], v[:half]], axis=0)

    def grad_body(x_blk, wqkv_blk, wout_blk, seg_blk, dy_blk):
        group = lax.axis_index('dp')
        r = lax.axis_index('row')
        c = lax.axis_index('col')
        y = r // 2
        n_tok, n_hid = x_blk.shape
        half_qkv = wqkv_blk.shape[1] // 2
        half_out = n_hid // 2
        quarter = n_hid // 4

        dy_pair = jnp.concatenate([dy_blk, to_row(dy_blk, 2)], axis=0)
        dy_all = jnp.concatenate([dy_pair, to_row(dy_pair, 1)], axis=0)
        seg_pair = jnp.concatenate([seg_blk, to_row(seg_blk, 2)], axis=0)
        seg_all = jnp.concatenate([seg_pair, to_row(seg_pair, 1)], axis=0)

        x_row = lax.all_gather(x_blk, 'col', axis=1, tiled=True)
        x_two = jnp.concatenate([x_row, to_row(x_row, 2)], axis=0)

        do_part = mm(dy_all, wout_blk, NT)
        do_tok = lax.psum_scatter(do_part, 'col', scatter_dimension=0, tiled=True).astype(bf16)
        y_tok = (r ^ ((c >> 1) | ((c & 1) << 1))) // 2
        do_own = turn(cols(do_tok, y_tok * half_out, half_out), 0)
        do_far = turn(cols(do_tok, (1 - y_tok) * half_out, half_out), 2)
        do_two = jnp.concatenate([do_own, do_far], axis=0)

        w_y = cols(wqkv_blk, y * half_qkv, half_qkv)
        w_o = cols(wqkv_blk, (1 - y) * half_qkv, half_qkv)
        w_sib = to_row(w_y, 1)
        got = [to_row(lax.dynamic_slice_in_dim(w_o, group * 2 * quarter + s * quarter, quarter, axis=0), 2) for s in range(2)]
        got_far = [to_other_group(g) for g in got]
        w_r2 = jnp.concatenate(got + got_far, axis=0)
        w_r3 = to_row(w_r2, 1)

        def hid(j):
            return cols(x_two, (r ^ j) * n_hid, n_hid)

        def hid_split(j):
            base = (r ^ j) * n_hid
            lo = cols(x_two, base + group * half_out, half_out)
            hi = cols(x_two, base + (1 - group) * half_out, half_out)
            return jnp.concatenate([lo, hi], axis=1)

        x_r = hid(0)
        x_s = hid(1)
        qkv = mm(x_r, w_y, NN) + mm(x_s, w_sib, NN) + mm(hid_split(2), w_r2, NN) + mm(hid_split(3), w_r3, NN)
        qkv = qkv.astype(bf16)
        qkv_sib = to_row(qkv, 1)
        x_sib = to_row(x_s, 1)

        seg_q, seg_k = seg_pair[:, None], seg_all[None, :]
        (o,) = attention(fwd_kernel, qkv, qkv_sib, seg_q, seg_k)
        o, do_two = lax.optimization_barrier((o, do_two))
        o_all = lax.all_gather(o, 'col', axis=1, tiled=True)
        dq, dkv_own, dkv_sib = attention(bwd_kernel, qkv, qkv_sib, seg_q, seg_k, do_two)
        dkv = (dkv_own + to_row(dkv_sib, 1)).astype(bf16)

        def token_halves(v):
            v = v.reshape(2, 2, n_tok // 2, v.shape[1])
            return [v[:, h].reshape(n_tok, v.shape[3]) for h in range(2)]

        def unite(q_part, kv_part):
            d = HEAD_DIM
            parts = []
            for h in range(half_out // d):
                parts += [q_part[:, d * h:d * h + d], kv_part[:, 2 * d * h:2 * d * h + 2 * d]]
            return jnp.concatenate(parts, axis=1)

        near = [unite(u, v) for u, v in zip(token_halves(dq), token_halves(dkv))]
        grad_x, near_all, far_all, x_half = [], [], [], []
        x_both = [token_halves(x_r), token_halves(x_sib)]
        for h in range(2):
            far = to_row(swap(near[h]), 2)
            d_y = jnp.concatenate([near[h], to_row(near[h], 1)], axis=0)
            d_o = jnp.concatenate([far, to_row(far, 1)], axis=0)
            dx_near = mm(d_y, w_y, NT)
            dx_far = mm(d_o, w_o, NT)
            dx_part = dx_near + dx_far
            dx_tok = lax.psum_scatter(dx_part, 'col', scatter_dimension=0, tiled=True).astype(bf16)
            grad_x.append(turn(dx_tok, 0))
            near_all.append(d_y)
            far_all.append(d_o)
            x_half.append(jnp.concatenate([x_both[0][h], x_both[1][h]], axis=0))
        grad_x = jnp.concatenate(grad_x, axis=0)

        def by_y(own, other):
            return jnp.where(y == 0, jnp.concatenate([own, other], axis=1), jnp.concatenate([other, own], axis=1))

        d_all = by_y(jnp.concatenate(near_all, axis=0), jnp.concatenate(far_all, axis=0))
        grad_wqkv = mm(jnp.concatenate(x_half, axis=0), d_all, TN).astype(bf16)

        o_to = [cols(o_all, (r ^ j) * half_out, half_out) for j in range(4)]
        o_y = jnp.concatenate([o_to[0], to_row(o_to[1], 1)], axis=0)
        o_o = jnp.concatenate([to_row(swap(o_to[2]), 2), to_row(swap(o_to[3]), 3)], axis=0)
        grad_wout = mm(by_y(o_y, o_o), dy_all, TN).astype(bf16)
        return grad_x, grad_wqkv, grad_wout


    return jax.shard_map(grad_body, mesh=mesh, in_specs=(tok_spec, mat_spec, mat_spec, seg_spec, tok_spec), out_specs=(tok_spec, tok_spec, tok_spec), check_vma=False)
```
